32 devices in a mesh: rep: 2 (over z, core), dp: 16 (over x, y).
Axes of the slice: x: 4, y: 4, z: 1, core: 2. Of those that a mesh axis runs over, the one named last changes fastest.
The devices are a block of a 4x4x8 slice.
Arguments:
- x: bfloat16 [32, 2048, 896], P(('rep', 'dp')), parts along dimension 0
- dy: bfloat16 [32, 2048, 896], P(('rep', 'dp')), parts along dimension 0
- wq: bfloat16 [2, 896, 896], P(None, 'dp')
- wk: bfloat16 [2, 896, 128], P(None, 'dp')
- wv: bfloat16 [2, 896, 128], P(None, 'dp')
- wo: bfloat16 [2, 896, 896], P(None, 'dp')
- w_gate: bfloat16 [2, 896, 2560], P(None, 'dp')
- w_up: bfloat16 [2, 896, 2560], P(None, 'dp')
- w_down: bfloat16 [2, 2560, 896], P(None, 'dp')
Outputs:
- output 1: bfloat16 [32, 2048, 896], P(('rep', 'dp')), parts along dimension 0
- output 2: bfloat16 [4, 896, 896], P('rep', 'dp'), parts along dimension 0
- output 3: bfloat16 [4, 896, 128], P('rep', 'dp'), parts along dimension 0
- output 4: bfloat16 [4, 896, 128], P('rep', 'dp'), parts along dimension 0
- output 5: bfloat16 [4, 896, 896], P('rep', 'dp'), parts along dimension 0
- output 6: bfloat16 [4, 896, 2560], P('rep', 'dp'), parts along dimension 0
- output 7: bfloat16 [4, 896, 2560], P('rep', 'dp'), parts along dimension 0
- output 8: bfloat16 [4, 2560, 896], P('rep', 'dp'), parts along dimension 0
There are 2 independent parts. The reference program is written for one: setup_inputs(seed, part) draws one part's arguments, and reference() takes and returns one part's arrays. A program takes and returns all parts, laid end to end along the dimension named above; an argument that names none is the same for every part.
All inputs are finite; a program needn't handle non-finite values.
Results may differ from the reference program's by a relative error of at most 0.027.
Values are sent between devices in bfloat16 or wider.
A program may use at most 768 MiB of HBM per device.

```python
import jax
import jax.numpy as jnp
from jax import lax

SEQUENCES = 16
TOKENS = 2048
D = 896
HEADS = 7
KV_HEADS = 1
HEAD = 128
FF = 2560
LAYERS = 2
THETA = 10000
NAMES = ("wq", "wk", "wv", "wo", "w_gate", "w_up", "w_down")
SHAPES = {
    "wq": (LAYERS, D, HEADS * HEAD),
    "wk": (LAYERS, D, KV_HEADS * HEAD),
    "wv": (LAYERS, D, KV_HEADS * HEAD),
    "wo": (LAYERS, HEADS * HEAD, D),
    "w_gate": (LAYERS, D, FF),
    "w_up": (LAYERS, D, FF),
    "w_down": (LAYERS, FF, D),
}


def bump(key, n, height):
    away = (jnp.arange(n, dtype=jnp.int32) - jax.random.randint(key, (), 0, n, jnp.int32)) % n
    return jnp.where(away < n // 8, height, 1.0)


def together(key, own, strength):
    shared = jax.random.normal(key, own.shape[1:], jnp.float32)
    return (own + strength * shared) * lax.rsqrt(1 + strength * strength)


def setup_inputs(seed: int = 0, part: int = 0) -> dict:
    kx, kdy, ka, kb, kz, kf, kh, kl, *keys = jax.random.split(jax.random.key(seed), 8 + 3 * len(NAMES))
    kx, kdy, ka, kb = (jax.random.fold_in(k, part) for k in (kx, kdy, ka, kb))
    kw, km, kv = (keys[i::3] for i in range(3))
    shape = (SEQUENCES, TOKENS, D)
    much_x, much_dy = jax.random.uniform(kz, (2,), jnp.float32, 0.0, 1.0)
    loud = 2.0 ** jax.random.uniform(jax.random.fold_in(kz, 1), (), jnp.float32, -1.0, 2.0)
    layers = 2.0 ** jax.random.uniform(kl, (LAYERS, 1, 1), jnp.float32, -1.0, 1.0)
    times = {"wq": 1.0, "wk": 1.0, "wv": 2.0, "wo": layers, "w_gate": 1.0, "w_up": bump(kh, FF, 4.0), "w_down": layers}
    x = together(ka, jax.random.normal(kx, shape, jnp.float32), much_x) * bump(kf, D, 4.0)
    dy = together(kb, jax.random.normal(kdy, shape, jnp.float32), much_dy)
    drawn = {"x": x.astype(jnp.bfloat16), "dy": (loud * dy * (SEQUENCES * TOKENS) ** -0.5).astype(jnp.bfloat16)}
    for key, name in zip(kw, NAMES, strict=True):
        drawn[name] = (jax.random.normal(key, SHAPES[name], jnp.float32) * SHAPES[name][1] ** -0.5 * times[name]).astype(jnp.bfloat16)
    return drawn


def matmul(a, w):
    return jnp.dot(a, w, preferred_element_type=jnp.float32).astype(jnp.bfloat16)


def normed(h):
    wide = h.astype(jnp.float32)
    scale = lax.rsqrt(jnp.mean(wide**2, -1, keepdims=True) + 1e-6)
    return (wide * scale).astype(jnp.bfloat16)


def turned(t, theta):
    half = t.shape[-1] // 2
    angle = jnp.arange(t.shape[0], dtype=jnp.float32)[:, None] * theta ** (-jnp.arange(half, dtype=jnp.float32) / half)
    cos, sin = jnp.cos(angle)[:, None], jnp.sin(angle)[:, None]
    a, b = t[..., :half].astype(jnp.float32), t[..., half:].astype(jnp.float32)
    return jnp.concatenate([a * cos - b * sin, b * cos + a * sin], -1).astype(jnp.bfloat16)


def seen_by(q, k, v):
    tokens, kv = q.shape[0], k.shape[1]
    q = q.reshape(tokens, kv, -1, q.shape[-1])
    scores = jnp.einsum("tgsd,ugd->gstu", q.astype(jnp.float32), k.astype(jnp.float32)) * q.shape[-1] ** -0.5
    place = jnp.arange(tokens)
    weights = jax.nn.softmax(jnp.where(place[:, None] >= place, scores, -jnp.inf), -1).astype(jnp.bfloat16)
    return jnp.einsum("gstu,ugd->tgsd", weights.astype(jnp.float32), v.astype(jnp.float32)).astype(jnp.bfloat16).reshape(tokens, -1)


def layer(h, w):
    a = normed(h)
    q, k = (turned(matmul(a, w[name]).reshape(h.shape[0], -1, HEAD), THETA) for name in ("wq", "wk"))
    h = h + matmul(seen_by(q, k, matmul(a, w["wv"]).reshape(h.shape[0], -1, HEAD)), w["wo"])
    b = normed(h)
    gate = jnp.dot(b, w["w_gate"], preferred_element_type=jnp.float32)
    up = jnp.dot(b, w["w_up"], preferred_element_type=jnp.float32)
    return h + matmul((jax.nn.silu(gate) * up).astype(jnp.bfloat16), w["w_down"])


def stack(weights, h):
    return lax.scan(lambda h, w: (layer(h, w), None), h, weights)[0]


def reference(x, dy, wq, wk, wv, wo, w_gate, w_up, w_down):
    weights = dict(zip(NAMES, (wq, wk, wv, wo, w_gate, w_up, w_down), strict=True))

    def take(so_far, sequence):
        h, by_y = sequence
        _, back = jax.vjp(stack, weights, h)
        by_weights, by_h = back(by_y)
        return jax.tree.map(lambda total, term: total + term.astype(jnp.float32), so_far, by_weights), by_h

    none_yet = {name: jnp.zeros(w.shape, jnp.float32) for name, w in weights.items()}
    by_weights, by_x = lax.scan(take, none_yet, (x, dy))
    return (by_x, *(by_weights[name].astype(jnp.bfloat16) for name in NAMES))
```

```python
import functools
import math

import jax
import jax.numpy as jnp
from jax import lax
from jax.experimental import pallas as pl
from jax.experimental.pallas import tpu as pltpu
from jax.sharding import PartitionSpec as P

HEAD = 128
THETA = 10000
EPS = 1e-6
LOG2E = 1.4426950408889634
SCALE = HEAD**-0.5
NEG = -1e30
HIDDEN = 2 * NEG
VMEM = 56 * 2**20
BF, F32 = jnp.bfloat16, jnp.float32


def _dot(a, b, ca, cb, **k):
    return lax.dot_general(a, b, (((ca,), (cb,)), ((), ())), preferred_element_type=F32, **k)


def _fit(size, want, unit=128):
    return max(n for n in range(unit, max(min(want, size), unit) + 1, unit) if size % n == 0)


def _params(*kinds):
    return pltpu.CompilerParams(dimension_semantics=kinds, vmem_limit_bytes=VMEM)


def _turn(t, cos, sin):
    wide = t.astype(F32)
    return (wide * cos + pltpu.roll(wide, HEAD // 2, 1) * sin).astype(BF)


def _gap(bk, bq):
    return lax.broadcasted_iota(jnp.int32, (bk, bq), 1) - lax.broadcasted_iota(jnp.int32, (bk, bq), 0)


def _attend_kernel(q_ref, k_ref, v_ref, cosq_ref, sinq_ref, cos_ref, sin_ref, o_ref, lse_ref, q_s, k_s, v_s, top_s, mix_s, *, bk):
    bq, g = q_ref.shape[0], q_ref.shape[1] // HEAD
    iq = pl.program_id(0)
    e = SCALE * LOG2E
    ones = jnp.ones((8, bk), BF)

    @pl.when(iq == 0)
    def _():
        k_s[...] = _turn(k_ref[...], cos_ref[...], sin_ref[...])
        v_s[...] = v_ref[...].T

    for n in range(g):
        q_s[n] = _turn(q_ref[:, n * HEAD : (n + 1) * HEAD], cosq_ref[...], sinq_ref[...])
    top_s[...] = jnp.full_like(top_s, NEG)
    mix_s[...] = jnp.zeros_like(mix_s)

    def block(j, masked):
        here = pl.ds(pl.multiple_of(j * bk, bk), bk)
        keys = k_s[here, :]
        scores = [_dot(keys, q_s[n], 1, 1) for n in range(g)]
        ok = _gap(bk, bq) >= j * bk - iq * bq if masked else None
        values = jnp.concatenate([v_s[:, here], ones], axis=0)
        weights, keeps = [], []
        for n, s in enumerate(scores):
            if masked:
                s = jnp.where(ok, s, HIDDEN)
            old = top_s[n : n + 1, :]
            top = jnp.maximum(old, s.max(axis=0, keepdims=True))
            top_s[n : n + 1, :] = top
            weights.append(jnp.exp2((s - top) * e).astype(BF))
            keeps.append(jnp.exp2((old - top) * e))
        for n, (p, keep) in enumerate(zip(weights, keeps)):
            mix_s[n] = mix_s[n] * keep + _dot(values, p, 1, 0)

    whole = lax.div(iq * bq + 1, bk)
    last = lax.div(iq * bq + bq - 1 + bk, bk)
    lax.fori_loop(0, whole, lambda j, _: block(j, False), None)
    lax.fori_loop(whole, last, lambda j, _: block(j, True), None)
    for n in range(g):
        total = mix_s[n, HEAD : HEAD + 1, :]
        o_ref[:, n * HEAD : (n + 1) * HEAD] = (mix_s[n, :HEAD, :] * (1 / total)).T.astype(BF)
        lse_ref[n : n + 1, :] = top_s[n : n + 1, :] * SCALE + jnp.log(total)


def attend(qkv, cos, sin, bq=512, bk=512):
    t, wide = qkv.shape
    g = wide // HEAD - 2
    bq, bk = _fit(t, bq), _fit(t, bk)
    rows = lambda i: (i, 0)
    once = lambda i: (0, 0)
    return pl.pallas_call(
        functools.partial(_attend_kernel, bk=bk),
        grid=(t // bq,),
        in_specs=[pl.BlockSpec((bq, g * HEAD), rows), pl.BlockSpec((t, HEAD), lambda i: (0, g)), pl.BlockSpec((t, HEAD), lambda i: (0, g + 1)),
                  pl.BlockSpec((bq, HEAD), rows), pl.BlockSpec((bq, HEAD), rows), pl.BlockSpec((t, HEAD), once), pl.BlockSpec((t, HEAD), once)],
        out_specs=[pl.BlockSpec((bq, g * HEAD), rows), pl.BlockSpec((g, bq), lambda i: (0, i))],
        out_shape=[jax.ShapeDtypeStruct((t, g * HEAD), BF), jax.ShapeDtypeStruct((g, t), F32)],
        scratch_shapes=[pltpu.VMEM((g, bq, HEAD), BF), pltpu.VMEM((t, HEAD), BF), pltpu.VMEM((HEAD, t), BF), pltpu.VMEM((g, bq), F32),
                        pltpu.VMEM((g, HEAD + 8, bq), F32)],
        compiler_params=_params("arbitrary"),
        cost_estimate=pl.CostEstimate(flops=4 * g * t * t * HEAD, transcendentals=g * t * t, bytes_accessed=2 * t * 2 * g * HEAD),
        name="attend",
    )(qkv, qkv, qkv, cos, sin, cos, sin)


def _attend_bwd_kernel(q_ref, k_ref, v_ref, do_ref, o_ref, lse_ref, cosq_ref, sinq_ref, cos_ref, sin_ref, dqkv_ref,
                       q_s, do_s, k_s, kt_s, lse_s, delta_s, dq_s, dk_s, dv_s, *, bk):
    bq, g = q_ref.shape[0], q_ref.shape[1] // HEAD
    iq = pl.program_id(0)
    e = SCALE * LOG2E

    @pl.when(iq == 0)
    def _():
        turned = _turn(k_ref[...], cos_ref[...], sin_ref[...])
        k_s[...] = turned
        kt_s[...] = turned.T
        dk_s[...] = jnp.zeros_like(dk_s)
        dv_s[...] = jnp.zeros_like(dv_s)

    ones = jnp.ones((8, HEAD), F32)
    for n in range(g):
        part = slice(n * HEAD, (n + 1) * HEAD)
        q_s[n] = _turn(q_ref[:, part], cosq_ref[...], sinq_ref[...])
        do_s[n] = do_ref[:, part]
        both = do_ref[:, part].astype(F32) * o_ref[:, part].astype(F32)
        delta_s[n : n + 1, :] = _dot(ones, both, 1, 1, precision=lax.Precision.HIGHEST)[0:1, :]
    lse_s[...] = lse_ref[...] * LOG2E
    dq_s[...] = jnp.zeros_like(dq_s)

    def block(j, masked):
        here = pl.ds(pl.multiple_of(j * bk, bk), bk)
        keys, values = k_s[here, :], v_ref[here, :]
        scores = [_dot(keys, q_s[n], 1, 1) for n in range(g)]
        dps = [_dot(values, do_s[n], 1, 1) for n in range(g)]
        ok = _gap(bk, bq) >= j * bk - iq * bq if masked else None
        for n in range(g):
            p = jnp.exp2(scores[n] * e - lse_s[n : n + 1, :])
            if masked:
                p = jnp.where(ok, p, 0.0)
            ds = (p * (dps[n] - delta_s[n : n + 1, :])).astype(BF)
            dv_s[here, :] += _dot(p.astype(BF), do_s[n], 1, 0)
            dk_s[here, :] += _dot(ds, q_s[n], 1, 0)
            dq_s[n] += _dot(kt_s[:, here], ds, 1, 0)

    whole = lax.div(iq * bq + 1, bk)
    last = lax.div(iq * bq + bq - 1 + bk, bk)
    lax.fori_loop(0, whole, lambda j, _: block(j, False), None)
    lax.fori_loop(whole, last, lambda j, _: block(j, True), None)
    rows = pl.ds(pl.multiple_of(iq * bq, bq), bq)
    for n in range(g):
        back = (dq_s[n] * SCALE).T.astype(BF)
        dqkv_ref[rows, n * HEAD : (n + 1) * HEAD] = _turn(back, cosq_ref[...], -sinq_ref[...])

    @pl.when(iq == pl.num_programs(0) - 1)
    def _():
        back = (dk_s[...] * SCALE).astype(BF)
        dqkv_ref[:, g * HEAD : (g + 1) * HEAD] = _turn(back, cos_ref[...], -sin_ref[...])
        dqkv_ref[:, (g + 1) * HEAD :] = dv_s[...].astype(BF)


def attend_bwd(qkv, o, lse, do, cos, sin, bq=512, bk=512):
    t, wide = qkv.shape
    g = wide // HEAD - 2
    bq, bk = _fit(t, bq), _fit(t, bk)
    rows = lambda i: (i, 0)
    once = lambda i: (0, 0)
    return pl.pallas_call(
        functools.partial(_attend_bwd_kernel, bk=bk),
        grid=(t // bq,),
        in_specs=[pl.BlockSpec((bq, g * HEAD), rows), pl.BlockSpec((t, HEAD), lambda i: (0, g)), pl.BlockSpec((t, HEAD), lambda i: (0, g + 1)),
                  pl.BlockSpec((bq, g * HEAD), rows), pl.BlockSpec((bq, g * HEAD), rows), pl.BlockSpec((g, bq), lambda i: (0, i)),
                  pl.BlockSpec((bq, HEAD), rows), pl.BlockSpec((bq, HEAD), rows), pl.BlockSpec((t, HEAD), once), pl.BlockSpec((t, HEAD), once)],
        out_specs=pl.BlockSpec((t, wide), once),
        out_shape=jax.ShapeDtypeStruct((t, wide), BF),
        scratch_shapes=[pltpu.VMEM((g, bq, HEAD), BF), pltpu.VMEM((g, bq, HEAD), BF), pltpu.VMEM((t, HEAD), BF), pltpu.VMEM((HEAD, t), BF),
                        pltpu.VMEM((g, bq), F32), pltpu.VMEM((g, bq), F32), pltpu.VMEM((g, HEAD, bq), F32), pltpu.VMEM((t, HEAD), F32),
                        pltpu.VMEM((t, HEAD), F32)],
        compiler_params=_params("arbitrary"),
        cost_estimate=pl.CostEstimate(flops=10 * g * t * t * HEAD, transcendentals=g * t * t, bytes_accessed=2 * t * 4 * g * HEAD),
        name="attend_bwd",
    )(qkv, qkv, qkv, do, o, lse, cos, sin, cos, sin)


STRIPE = 256


def _mix_kernel(*refs, layers, apart):
    for n in range(layers):
        gate, up = (ref.at[n] for ref in (refs[-2:] if apart else refs[:2]))
        both = refs[n] if apart else refs[2 + n]
        for at in range(0, gate.shape[1], STRIPE):
            for ref, to in ((gate, 2 * at), (up, 2 * at + STRIPE)):
                if apart:
                    ref[:, at : at + STRIPE] = both[:, to : to + STRIPE]
                else:
                    both[:, to : to + STRIPE] = ref[:, at : at + STRIPE]


def mixed(gate, up):
    layers, rows, ff = gate.shape
    return pl.pallas_call(functools.partial(_mix_kernel, layers=layers, apart=False),
                          out_shape=[jax.ShapeDtypeStruct((rows, 2 * ff), BF)] * layers, name="mixed")(gate, up)


def unmixed(both):
    rows, wide = both[0].shape
    return pl.pallas_call(functools.partial(_mix_kernel, layers=len(both), apart=True),
                          out_shape=[jax.ShapeDtypeStruct((len(both), rows, wide // 2), BF)] * 2, name="unmixed")(*both)


def _gated_kernel(b_ref, w_ref, gu_ref, act_ref, *, rows):
    for at in range(0, b_ref.shape[0], rows):
        both = _dot(b_ref[at : at + rows, :], w_ref[...], 1, 0)
        gu_ref[at : at + rows, :] = both
        gate, up = both[:, :STRIPE], both[:, STRIPE:]
        act_ref[at : at + rows, :] = (gate * jax.nn.sigmoid(gate) * up).astype(BF)


def gated(b, w_gu, rows=256):
    t, d = b.shape
    ff = w_gu.shape[1] // 2
    rows = _fit(t, rows)
    stripe = lambda j: (0, j)
    return pl.pallas_call(
        functools.partial(_gated_kernel, rows=rows),
        grid=(ff // STRIPE,),
        in_specs=[pl.BlockSpec((t, d), lambda j: (0, 0)), pl.BlockSpec((d, 2 * STRIPE), stripe)],
        out_specs=[pl.BlockSpec((t, 2 * STRIPE), stripe), pl.BlockSpec((t, STRIPE), stripe)],
        out_shape=[jax.ShapeDtypeStruct((t, 2 * ff), F32), jax.ShapeDtypeStruct((t, ff), BF)],
        compiler_params=_params("arbitrary"),
        cost_estimate=pl.CostEstimate(flops=4 * t * d * ff, transcendentals=t * ff, bytes_accessed=10 * t * ff + 4 * d * ff + 2 * t * d),
        name="gated",
    )(b, w_gu)


def _gated_bwd_kernel(g_ref, wd_ref, gu_ref, dgu_ref, *, rows):
    for at in range(0, g_ref.shape[0], rows):
        here = slice(at, at + rows)
        back = _dot(g_ref[here, :], wd_ref[...], 1, 1).astype(BF).astype(F32)
        gate, up = gu_ref[here, :STRIPE], gu_ref[here, STRIPE:]
        sig = jax.nn.sigmoid(gate)
        dgu_ref[here, :STRIPE] = (back * up * (sig * (1 + gate * (1 - sig)))).astype(BF)
        dgu_ref[here, STRIPE:] = (back * (gate * sig)).astype(BF)


def gated_bwd(g, w_down, gu, rows=256):
    t, d = g.shape
    ff = w_down.shape[0]
    rows = _fit(t, rows)
    stripe = pl.BlockSpec((t, 2 * STRIPE), lambda j: (0, j))
    return pl.pallas_call(
        functools.partial(_gated_bwd_kernel, rows=rows),
        grid=(ff // STRIPE,),
        in_specs=[pl.BlockSpec((t, d), lambda j: (0, 0)), pl.BlockSpec((STRIPE, d), lambda j: (j, 0)), stripe],
        out_specs=stripe,
        out_shape=jax.ShapeDtypeStruct((t, 2 * ff), BF),
        compiler_params=_params("arbitrary"),
        cost_estimate=pl.CostEstimate(flops=2 * t * d * ff, transcendentals=t * ff, bytes_accessed=12 * t * ff + 2 * d * ff + 2 * t * d),
        name="gated_bwd",
    )(g, w_down, gu)


def _into_norm_kernel(d_ref, w_ref, h_ref, g_ref, out_ref, *sums, rows, steps):
    k = pl.program_id(0)

    def finish(at, by_b):
        by_b = by_b.astype(BF).astype(F32)
        wide = h_ref[at, :].astype(F32)
        s = lax.rsqrt(jnp.mean(wide * wide, -1, keepdims=True) + EPS)
        back = by_b * s - wide * (s * s * s * jnp.mean(by_b * wide, -1, keepdims=True))
        out_ref[at, :] = (g_ref[at, :].astype(F32) + back.astype(BF).astype(F32)).astype(BF)

    places = [slice(at, at + rows) for at in range(0, h_ref.shape[0], rows)]
    if steps == 1:
        for at in places:
            finish(at, _dot(d_ref[at, :], w_ref[...], 1, 1))
        return
    sum_s = sums[0]

    @pl.when(k == 0)
    def _():
        for at in places:
            sum_s[at, :] = _dot(d_ref[at, :], w_ref[...], 1, 1)

    @pl.when((k > 0) & (k < steps - 1))
    def _():
        for at in places:
            sum_s[at, :] += _dot(d_ref[at, :], w_ref[...], 1, 1)

    @pl.when(k == steps - 1)
    def _():
        for at in places:
            finish(at, sum_s[at, :] + _dot(d_ref[at, :], w_ref[...], 1, 1))


def into_norm(d, w, h, g, cols, rows=256):
    t, n = d.shape
    width = w.shape[0]
    rows, cols = _fit(t, rows), _fit(n, cols)
    steps = n // cols
    once = pl.BlockSpec((t, width), lambda k: (0, 0))
    return pl.pallas_call(
        functools.partial(_into_norm_kernel, rows=rows, steps=steps),
        grid=(steps,),
        in_specs=[pl.BlockSpec((t, cols), lambda k: (0, k)), pl.BlockSpec((width, cols), lambda k: (0, k)), once, once],
        out_specs=once,
        out_shape=jax.ShapeDtypeStruct((t, width), BF),
        scratch_shapes=[pltpu.VMEM((t, width), F32)] if steps > 1 else [],
        compiler_params=_params("arbitrary"),
        cost_estimate=pl.CostEstimate(flops=2 * t * width * n, transcendentals=t, bytes_accessed=2 * (n * (t + width) + 3 * t * width)),
        name="into_norm",
    )(d, w, h, g)


MESH = pl.DeviceIdType.MESH


def _place(axis, side):
    me = lax.axis_index("dp")
    x, y = lax.div(me, side), lax.rem(me, side)
    if axis == 0:
        return x, lambda by: lax.rem(x + by + side, side) * side + y
    return y, lambda by: x * side + lax.rem(y + by + side, side)


def _greet(side):
    barrier = pltpu.get_barrier_semaphore()
    for axis in (0, 1):
        _, there = _place(axis, side)
        for by in (1, -1):
            pl.semaphore_signal(barrier, inc=1, device_id={"dp": there(by)}, device_id_type=MESH)
    pl.semaphore_wait(barrier, 4)


def _send(src, dst, sems, number, to):
    copy = pltpu.make_async_remote_copy(src_ref=src, dst_ref=dst, send_sem=sems[0].at[number], recv_sem=sems[1].at[number],
                                        device_id={"dp": to}, device_id_type=MESH)
    copy.start()
    return copy


def _gather_kernel(a_ref, b_ref, oa_ref, ob_ref, send_a, recv_a, send_b, recv_b, own_sem, *, side):
    _greet(side)
    todo = []
    for k, (ref, out, sems) in enumerate(((a_ref, oa_ref, (send_a, recv_a)), (b_ref, ob_ref, (send_b, recv_b)))):
        p1, to1 = _place(k, side)
        p2, to2 = _place(1 - k, side)
        half = ref.shape[1] // 2
        slot = (lambda i, j, out=out: out.at[i, j]) if k == 0 else (lambda i, j, out=out: out.at[j, i])
        line = (lambda j, at, out=out: out.at[at, j]) if k == 0 else (lambda j, at, out=out: out.at[j, at])
        todo.append((ref, out, sems, p1, to1, p2, to2, half, slot, line, k))
    sent, own = [], []
    step = []
    for ref, out, sems, p1, to1, p2, to2, half, slot, line, k in todo:
        up, down = _send(ref, slot(p1, p2), sems, 0, to1(1)), _send(ref, slot(p1, p2), sems, 1, to1(-1))
        mine = pltpu.make_async_copy(ref, slot(p1, p2), own_sem.at[k])
        mine.start()
        step.append((up, down))
        sent += [up, down]
        own.append(mine)
    then = []
    for (ref, out, sems, p1, to1, p2, to2, half, slot, line, k), (up, down) in zip(todo, step):
        before, behind = lax.rem(p1 + side - 1, side), lax.rem(p1 + 1, side)
        up.wait_recv()
        one = slot(before, p2).at[:, :half]
        up = _send(one, one, sems, 2, to1(1))
        down.wait_recv()
        two = slot(behind, p2).at[:, half:]
        down = _send(two, two, sems, 3, to1(-1))
        then.append((up, down))
        sent += [up, down]
    step = []
    for (ref, out, sems, p1, to1, p2, to2, half, slot, line, k), (up, down), mine in zip(todo, then, own):
        up.wait_recv()
        down.wait_recv()
        mine.wait()
        whole = line(p2, slice(None))
        up, down = _send(whole, whole, sems, 4, to2(1)), _send(whole, whole, sems, 5, to2(-1))
        step.append((up, down))
        sent += [up, down]
    then = []
    for (ref, out, sems, p1, to1, p2, to2, half, slot, line, k), (up, down) in zip(todo, step):
        before, behind = lax.rem(p2 + side - 1, side), lax.rem(p2 + 1, side)
        up.wait_recv()
        one = line(before, pl.ds(0, side // 2))
        up = _send(one, one, sems, 6, to2(1))
        down.wait_recv()
        two = line(behind, pl.ds(side // 2, side // 2))
        down = _send(two, two, sems, 7, to2(-1))
        then.append((up, down))
        sent += [up, down]
    for up, down in then:
        up.wait_recv()
        down.wait_recv()
    for copy in sent:
        copy.wait_send()


def gather_pair(a, b, n):
    side = math.isqrt(n)
    outs = [jax.ShapeDtypeStruct((side, side) + w.shape, w.dtype) for w in (a, b)]
    near, far = pl.BlockSpec(memory_space=pltpu.VMEM), pl.BlockSpec(memory_space=pl.ANY)
    got = pl.pallas_call(
        functools.partial(_gather_kernel, side=side),
        in_specs=[near, near],
        out_specs=[far, far],
        out_shape=outs,
        scratch_shapes=[pltpu.SemaphoreType.DMA((8,))] * 4 + [pltpu.SemaphoreType.DMA((2,))],
        compiler_params=pltpu.CompilerParams(collective_id=0, has_side_effects=True),
        cost_estimate=pl.CostEstimate(flops=2**32, transcendentals=0, bytes_accessed=n * 4 * a.size),
        name="gather_pair",
    )(a, b)
    return [t.reshape(n * w.shape[0], w.shape[1]) for t, w in zip(got, (a, b))]


def _scatter_kernel(a_ref, b_ref, oa_ref, ob_ref, ra, ta, fa, ga, qa, ua, rb, tb, fb, gb, qb, ub, send_a, recv_a, send_b, recv_b, *, side):
    _greet(side)
    wide = lambda t: t.astype(F32)
    todo = []
    for k, it in enumerate(((a_ref, oa_ref, ra, ta, fa, ga, qa, ua, (send_a, recv_a)), (b_ref, ob_ref, rb, tb, fb, gb, qb, ub, (send_b, recv_b)))):
        g_ref = it[0]
        p1, to1 = _place(k, side)
        p2, to2 = _place(1 - k, side)
        two = side // 2
        if k == 0:
            piece = lambda i, h, g_ref=g_ref: g_ref.at[i, pl.ds(two * h, two)]
            block = lambda i, j, g_ref=g_ref: g_ref[i, j]
        else:
            piece = lambda i, h, g_ref=g_ref: g_ref.at[pl.ds(two * h, two), i]
            block = lambda i, j, g_ref=g_ref: g_ref[j, i]
        todo.append((*it, p1, to1, p2, to2, piece, block, -(-g_ref.shape[3] // 256) * 128))
    on = lambda p, by: lax.rem(p + by + side, side)
    two = side // 2
    sent, step = [], []
    for g_ref, o_ref, r, t, f, gl, q, u, sems, p1, to1, p2, to2, piece, block, cut in todo:
        step.append([_send(piece(on(p1, 2), 0), r.at[0], sems, 0, to1(1)), _send(piece(on(p1, 2), 1), r.at[1], sems, 1, to1(-1)),
                     _send(piece(on(p1, 1), 1), r.at[2], sems, 2, to1(1)), _send(piece(on(p1, -1), 0), r.at[3], sems, 3, to1(-1))])
    for (g_ref, o_ref, r, t, f, gl, q, u, sems, p1, to1, p2, to2, piece, block, cut), copies in zip(todo, step):
        copies[0].wait_recv()
        for j in range(two):
            t[0, j] = (wide(block(on(p1, 1), j)) + wide(r[0, j])).astype(BF)
        copies.append(_send(t.at[0], r.at[4], sems, 4, to1(1)))
        copies[1].wait_recv()
        for j in range(two):
            t[1, j] = (wide(block(on(p1, -1), two + j)) + wide(r[1, j])).astype(BF)
        copies.append(_send(t.at[1], r.at[5], sems, 5, to1(-1)))
    onward = []
    for (g_ref, o_ref, r, t, f, gl, q, u, sems, p1, to1, p2, to2, piece, block, cut), copies in zip(todo, step):
        for copy in copies[2:]:
            copy.wait_recv()
        for j in range(two):
            low = wide(block(p1, j)) + (wide(r[4, j]) + wide(r[3, j]))
            high = wide(block(p1, two + j)) + (wide(r[5, j]) + wide(r[2, j]))
            f[j], f[two + j] = low, high
            gl[j], gl[two + j] = low.astype(BF), high.astype(BF)
        left, right = slice(0, cut), slice(cut, g_ref.shape[3])
        onward.append([_send(gl.at[on(p2, 2), :, left], q.at[0, :, left], sems, 6, to2(1)),
                       _send(gl.at[on(p2, 2), :, right], q.at[1, :, right], sems, 7, to2(-1)),
                       _send(gl.at[on(p2, 1), :, right], q.at[2, :, right], sems, 8, to2(1)),
                       _send(gl.at[on(p2, -1), :, left], q.at[3, :, left], sems, 9, to2(-1))])
    for (g_ref, o_ref, r, t, f, gl, q, u, sems, p1, to1, p2, to2, piece, block, cut), copies in zip(todo, onward):
        left, right = slice(0, cut), slice(cut, g_ref.shape[3])
        copies[0].wait_recv()
        u[:, left] = (f[on(p2, 1), :, left] + wide(q[0, :, left])).astype(BF)
        copies.append(_send(u.at[:, left], q.at[4, :, left], sems, 10, to2(1)))
        copies[1].wait_recv()
        u[:, right] = (f[on(p2, -1), :, right] + wide(q[1, :, right])).astype(BF)
        copies.append(_send(u.at[:, right], q.at[5, :, right], sems, 11, to2(-1)))
    for (g_ref, o_ref, r, t, f, gl, q, u, sems, p1, to1, p2, to2, piece, block, cut), copies in zip(todo, onward):
        left, right = slice(0, cut), slice(cut, g_ref.shape[3])
        for copy in copies[2:]:
            copy.wait_recv()
        o_ref[:, left] = (f[p2, :, left] + (wide(q[4, :, left]) + wide(q[3, :, left]))).astype(BF)
        o_ref[:, right] = (f[p2, :, right] + (wide(q[5, :, right]) + wide(q[2, :, right]))).astype(BF)
    for copies in step + onward:
        for copy in copies:
            copy.wait_send()


def scatter_pair(a, b, n):
    side = math.isqrt(n)
    near = pl.BlockSpec(memory_space=pltpu.VMEM)
    scratch, given = [], []
    for w in (a, b):
        rows, cols = w.shape[0] // n, w.shape[1]
        given.append(w.reshape(side, side, rows, cols))
        scratch += [pltpu.VMEM((6, side // 2, rows, cols), BF), pltpu.VMEM((2, side // 2, rows, cols), BF), pltpu.VMEM((side, rows, cols), F32),
                    pltpu.VMEM((side, rows, cols), BF), pltpu.VMEM((6, rows, cols), BF), pltpu.VMEM((rows, cols), BF)]
    return pl.pallas_call(
        functools.partial(_scatter_kernel, side=side),
        in_specs=[near, near],
        out_specs=[near, near],
        out_shape=[jax.ShapeDtypeStruct((w.shape[0] // n, w.shape[1]), BF) for w in (a, b)],
        scratch_shapes=scratch + [pltpu.SemaphoreType.DMA((12,))] * 4,
        compiler_params=pltpu.CompilerParams(collective_id=1, has_side_effects=True, vmem_limit_bytes=VMEM),
        cost_estimate=pl.CostEstimate(flops=2**32, transcendentals=0, bytes_accessed=4 * a.size + 4 * b.size),
        name="scatter_pair",
    )(*given)


def matmul(a, w):
    return jnp.dot(a, w, preferred_element_type=F32).astype(BF)


def matmul_t(a, w):
    return _dot(a, w, 1, 1).astype(BF)


def by_weight(a, d):
    return _dot(a, d, 0, 0).astype(BF)


def normed(h):
    wide = h.astype(F32)
    return (wide * lax.rsqrt(jnp.mean(wide**2, -1, keepdims=True) + EPS)).astype(BF)


def angles(tokens):
    half = HEAD // 2
    angle = jnp.arange(tokens, dtype=F32)[:, None] * THETA ** (-jnp.arange(half, dtype=F32) / half)
    cos, sin = jnp.cos(angle), jnp.sin(angle)
    return jnp.concatenate([cos, cos], -1), jnp.concatenate([-sin, sin], -1)


def after(first, *rest):
    return lax.optimization_barrier((first, *rest))[1:]


def solution(mesh):
    n_dp = mesh.shape["dp"]
    gather = lambda w: lax.all_gather(w, "dp", axis=0, tiled=True)
    scatter = lambda g: lax.psum_scatter(g, "dp", scatter_dimension=0, tiled=True)

    def step(x, dy, wq, wk, wv, wo, w_gate, w_up, w_down):
        layers, d = wq.shape[0], wq.shape[2]
        h, g = x[0], dy[0]
        wide = d + wk.shape[2] + wv.shape[2]
        near = [jnp.concatenate([w[n] for w in (wq, wk, wv, wo)], -1) for n in range(layers)]
        near = gather_pair(*near, n_dp)
        far = [(gather(w), gather(w_down[n])) for n, w in enumerate(mixed(w_gate, w_up))]
        cos, sin = angles(h.shape[0])
        kept = []
        for n in range(layers):
            w_qkv, w_o = near[n][:, :wide], near[n][:, wide:]
            w_gu, w_d = far[n]
            a = normed(h)
            qkv = matmul(a, w_qkv)
            o, lse = attend(qkv, cos, sin)
            mid = h + matmul(o, w_o)
            b = normed(mid)
            gu, act = gated(b, w_gu)
            kept.append((h, a, qkv, o, lse, mid, b, gu, act, w_qkv, w_o, w_gu, w_d))
            h = mid + matmul(act, w_d)
        mine = [[] for _ in range(layers)]
        for n in reversed(range(layers)):
            h, a, qkv, o, lse, mid, b, gu, act, w_qkv, w_o, w_gu, w_d = kept[n]
            before = mine[n + 1] if n + 1 < layers else [None] * 4
            by_d = by_weight(act, g)
            g, before[0] = lax.optimization_barrier((g, by_d, before[0]))[::2]
            got_d = scatter(by_d)
            dgu = gated_bwd(g, w_d, gu)
            by_gu = by_weight(b, dgu)
            dgu, before[1] = lax.optimization_barrier((dgu, by_gu, before[1]))[::2]
            got_gu = scatter(by_gu)
            g = into_norm(dgu, w_gu, mid, g, 1024)
            by_o = by_weight(o, g)
            do = matmul_t(g, w_o)
            dqkv = attend_bwd(qkv, o, lse, do, cos, sin)
            by_qkv = by_weight(a, dqkv)
            if n == 0:
                (dqkv,) = after(by_qkv, dqkv)
                g = into_norm(dqkv, w_qkv, h, g, wide)
                got_o, got_qkv = scatter_pair(by_o, by_qkv, n_dp)
            else:
                got_o, got_qkv = scatter_pair(by_o, by_qkv, n_dp)
                g = into_norm(dqkv, w_qkv, h, g, wide)
            mine[n] = [got_d, got_gu, got_o, got_qkv]
        g, mine = lax.optimization_barrier((g, mine))
        by_d, by_gu, by_o, by_qkv = zip(*mine, strict=True)
        by_q, by_k, by_v = jnp.split(jnp.stack(by_qkv), [d, d + wk.shape[2]], -1)
        by_gate, by_up = unmixed(by_gu)
        return g[None], by_q, by_k, by_v, jnp.stack(by_o), by_gate, by_up, jnp.stack(by_d)

    states, cut = P(("rep", "dp"), None, None), P(None, "dp", None)
    return jax.shard_map(
        step,
        mesh=mesh,
        in_specs=(states, states) + (cut,) * 7,
        out_specs=(states,) + (P("rep", "dp", None),) * 7,
        check_vma=False,
    )
```
